32 devices in a mesh: scan: 2 (over y), angle: 16 (over z, x, core).
Axes of the slice: x: 2, y: 2, z: 4, core: 2. Of those that a mesh axis runs over, the one named last changes fastest.
Arguments:
- object_init: float32 [32, 2, 128, 1024], P(('scan', 'angle')), parts along dimension 0, may hold values from -3.6 to 3.6
- measured: bfloat16 [32, 15, 128, 128], P(('scan', 'angle')), parts along dimension 0
- positions: int32 [32, 15, 2], P(('scan', 'angle')), parts along dimension 0, may hold values from 0 to 896, as said below
- angle_list: int32 [32], P('scan'), parts along dimension 0, may hold values from 0 to 15, each once
- probe: float32 [4, 128, 128], P('scan'), parts along dimension 0, may hold values from -3 to 3
- radial: float32 [16, 1024, 1024], P('angle'), may hold values from -0.1875 to 0.1875
Outputs:
- slices: float32 [32, 2, 128, 1024], P(('scan', 'angle')), parts along dimension 0
- probe_out: float32 [4, 128, 128], P('scan'), parts along dimension 0
The draws below stay inside these ranges and needn't reach their ends.
There are 2 independent parts, one for each index of `scan`. The reference program is written for one: setup_inputs(seed, part) draws one part's arguments, and reference() takes and returns one part's arrays. A program takes and returns all parts, laid end to end along the dimension named above; an argument that names none is the same for every part. Nothing has to cross between parts.
Inputs may be any that keep to these rules, and one draw needn't show every extreme that they name: `positions`: for each angle, patch number n = r * 15 + c has offsets (r * 64, c * 64) moved by at most 8 cells in each dimension and clipped so that the patch lies inside the 128 x 1024 projection.
All inputs are finite; a program needn't handle non-finite values.
Results may differ from the reference program's by a relative error of at most 0.0014.
The reference program's roundings to bfloat16 on the way count: a program that leaves them out, or rounds other values in their place, can miss the bound.
Values sent between devices are 32-bit elements; how exact they have to be, the bound alone decides.
A program may use at most 64 MiB of HBM per device.

```python
import math
import jax
import jax.numpy as jnp
from jax import lax

PATCH = 128
NC = 1024
ROWS = 128
ITERS = 2
ANG = 16


def draw_positions(key, part):
    patch_rows = 2 * ROWS // PATCH - 1
    patch_cols = 2 * NC // PATCH - 1
    index = jnp.arange(patch_rows * patch_cols, dtype=jnp.int32)
    base_row = index // patch_cols * (PATCH // 2)
    base_col = index % patch_cols * (PATCH // 2)
    reach = PATCH // 16
    jitter = jax.random.randint(jax.random.fold_in(key, 11), (ANG, patch_rows * patch_cols, 2), -reach, reach + 1)
    row_at = jnp.clip(base_row[None, :] + jitter[:, :, 0], 0, ROWS - PATCH)
    col_at = jnp.clip(base_col[None, :] + jitter[:, :, 1], 0, NC - PATCH)
    return jnp.stack([row_at, col_at], -1).astype(jnp.int32)


def truth_fields(key):
    ramp = jnp.arange(ANG, dtype=jnp.float32) / max(ANG - 1, 1)
    power = 0.55 * jnp.power(3.0, ramp)
    amplitude = jnp.sqrt(power)[:, None, None, None]
    true_obj = amplitude * 0.7 * jax.random.truncated_normal(jax.random.fold_in(key, 31), -3.0, 3.0, (ANG, 2, ROWS, NC), jnp.float32)
    true_prb = 0.5 * jax.random.truncated_normal(jax.random.fold_in(key, 37), -3.0, 3.0, (2, PATCH, PATCH), jnp.float32)
    return (true_obj, true_prb)


def perturbation(key, shape, spread):
    return spread * jax.random.truncated_normal(key, -3.0, 3.0, shape, jnp.float32)


def draw_object_init(key, part):
    true_obj, true_prb = truth_fields(key)
    return true_obj + perturbation(jax.random.fold_in(key, 41), true_obj.shape, 0.3)


def draw_probe(key, part):
    true_obj, true_prb = truth_fields(key)
    return true_prb + perturbation(jax.random.fold_in(key, 43), true_prb.shape, 0.45)


def spectral_tables(count):
    index = jnp.arange(count, dtype=jnp.int32)
    phase = index[:, None] * index[None, :] % count
    angle = phase.astype(jnp.float32) * (2.0 * math.pi / count)
    scale = 1.0 / math.sqrt(count)
    return (jnp.cos(angle) * scale, jnp.sin(angle) * scale)


def draw_measured(key, part):
    true_obj, true_prb = truth_fields(key)
    offsets = draw_positions(key, part)
    cosine_theta, sine_theta = spectral_tables(PATCH)
    exact = lax.Precision.HIGHEST
    zero_index = jnp.zeros((), jnp.int32)

    def intensity(items):
        field, scan_positions = items
        pieces = jax.vmap(lambda row, col: lax.dynamic_slice(field, (zero_index, row, col), (2, PATCH, PATCH)))(scan_positions[:, 0], scan_positions[:, 1])
        piece_re, piece_im = (pieces[:, 0], pieces[:, 1])
        wave_re = true_prb[0] * piece_re - true_prb[1] * piece_im
        wave_im = true_prb[0] * piece_im + true_prb[1] * piece_re
        half_re = jnp.einsum('jk,nkl->njl', cosine_theta, wave_re, precision=exact) + jnp.einsum('jk,nkl->njl', sine_theta, wave_im, precision=exact)
        half_im = jnp.einsum('jk,nkl->njl', cosine_theta, wave_im, precision=exact) - jnp.einsum('jk,nkl->njl', sine_theta, wave_re, precision=exact)
        farfield_real = jnp.einsum('njk,kl->njl', half_re, cosine_theta, precision=exact) + jnp.einsum('njk,kl->njl', half_im, sine_theta, precision=exact)
        farfield_imaginary = jnp.einsum('njk,kl->njl', half_im, cosine_theta, precision=exact) - jnp.einsum('njk,kl->njl', half_re, sine_theta, precision=exact)
        return farfield_real * farfield_real + farfield_imaginary * farfield_imaginary
    return lax.map(intensity, (true_obj, offsets)).astype(jnp.bfloat16)


def block_scale(key, extent, cuts, least, top_value):
    factor_of, own = 1.0, jax.random.fold_in(key, 6)
    for position, shards_of in cuts:
        heights = jnp.exp(jax.random.uniform(jax.random.fold_in(own, position), (shards_of,), jnp.float32, least / len(cuts), top_value / len(cuts)))
        factor_of = factor_of * jnp.repeat(heights, extent[position] // shards_of).reshape([-1 if axis == position else 1 for axis in range(len(extent))])
    return factor_of


def normal_values(rng, dims, scale, limit, shards=(), kind=jnp.bfloat16):
    factor_of = block_scale(rng, dims, shards, -0.22, 0.18) if shards else 1.0
    drawn = jax.random.normal(rng, dims, jnp.float32) * scale * factor_of
    return jnp.minimum(jnp.maximum(drawn, -limit), limit).astype(kind)


def setup_inputs(seed: int = 0, part: int = 0) -> dict:
    streams_of = jax.random.split(jax.random.key(seed), 7)
    own_keys = jax.random.split(jax.random.fold_in(streams_of[6], part), 7)
    object_init = draw_object_init(jax.random.fold_in(jax.random.fold_in(streams_of[6], part), 71), part)
    measured = draw_measured(jax.random.fold_in(jax.random.fold_in(streams_of[6], part), 71), part)
    positions = draw_positions(jax.random.fold_in(jax.random.fold_in(streams_of[6], part), 71), part)
    angle_list = jax.random.permutation(own_keys[3], ANG).astype(jnp.int32)
    probe = draw_probe(jax.random.fold_in(jax.random.fold_in(streams_of[6], part), 71), part)
    radial = normal_values(streams_of[5], (ANG, NC, NC), NC ** -0.5, 0.1875, ((0, 16),), jnp.float32)
    return {"object_init": object_init, "measured": measured, "positions": positions, "angle_list": angle_list, "probe": probe, "radial": radial}


object_rate = 0.5
probe_rate = 1.0

def tables_exact(count, index_list):
    index = jnp.arange(count, dtype=jnp.int32)
    phase = index[:, None] * index_list[None, :] % count
    angle = phase.astype(jnp.float32) * (2.0 * math.pi / count)
    scale = 1.0 / math.sqrt(count)
    return (jnp.cos(angle) * scale, jnp.sin(angle) * scale)

def tables(count, index_list):
    cosine_part, sine_part = tables_exact(count, index_list)
    return (cosine_part.astype(jnp.bfloat16), sine_part.astype(jnp.bfloat16))

def left(table, field):
    return jnp.einsum('jk,nkl->njl', table.astype(jnp.float32), field.astype(jnp.float32))

def right(field, table):
    return jnp.einsum('njk,kl->njl', field.astype(jnp.float32), table.astype(jnp.float32))

def gradient_list(object_field, measured_intensity, scan_positions, probe_field, cosine_theta, sine_theta):
    size = probe_field.shape[1]
    zero_index = jnp.zeros((), jnp.int32)
    pieces = jax.vmap(lambda row, col: lax.dynamic_slice(object_field, (zero_index, row, col), (2, size, size)))(scan_positions[:, 0], scan_positions[:, 1])
    piece_re, piece_im = (pieces[:, 0], pieces[:, 1])
    probe_re, probe_im = (probe_field[0], probe_field[1])
    wave_re = (probe_re * piece_re - probe_im * piece_im).astype(jnp.bfloat16)
    wave_im = (probe_re * piece_im + probe_im * piece_re).astype(jnp.bfloat16)
    half_re = (left(cosine_theta, wave_re) + left(sine_theta, wave_im)).astype(jnp.bfloat16)
    half_im = (left(cosine_theta, wave_im) - left(sine_theta, wave_re)).astype(jnp.bfloat16)
    farfield_real = right(half_re, cosine_theta) + right(half_im, sine_theta)
    farfield_imaginary = right(half_im, cosine_theta) - right(half_re, sine_theta)
    residual_error = farfield_real * farfield_real + farfield_imaginary * farfield_imaginary - measured_intensity.astype(jnp.float32)
    push_re = (residual_error * farfield_real).astype(jnp.bfloat16)
    push_im = (residual_error * farfield_imaginary).astype(jnp.bfloat16)
    back_re = (left(cosine_theta, push_re) - left(sine_theta, push_im)).astype(jnp.bfloat16)
    back_im = (left(cosine_theta, push_im) + left(sine_theta, push_re)).astype(jnp.bfloat16)
    grad_re = right(back_re, cosine_theta) - right(back_im, sine_theta)
    grad_im = right(back_im, cosine_theta) + right(back_re, sine_theta)
    step_re = probe_re * grad_re + probe_im * grad_im
    step_im = probe_re * grad_im - probe_im * grad_re
    steps_all = jnp.stack([step_re, step_im], 1)

    def place(index, total):
        start = (zero_index, scan_positions[index, 0], scan_positions[index, 1])
        current = lax.dynamic_slice(total, start, (2, size, size))
        return lax.dynamic_update_slice(total, current + steps_all[index], start)
    obj_grad = lax.fori_loop(0, scan_positions.shape[0], place, jnp.zeros_like(object_field))
    pg_re = lax.optimization_barrier(jnp.sum(piece_re * grad_re + piece_im * grad_im, 0))
    pg_im = lax.optimization_barrier(jnp.sum(piece_re * grad_im - piece_im * grad_re, 0))
    energy = jnp.sum(piece_re * piece_re + piece_im * piece_im)
    return (obj_grad, jnp.stack([pg_re, pg_im], 0), energy)

def reference(object_init, measured, positions, angle_list, probe, radial):
    size = probe.shape[1]
    cosine_theta, sine_theta = tables(size, jnp.arange(size, dtype=jnp.int32))
    object_field = object_init
    probe_field = probe
    for step in range(ITERS):

        def one(items):
            return gradient_list(items[0], items[1], items[2], probe_field, cosine_theta, sine_theta)
        obj_grads, probe_grads, energies = lax.map(one, (object_field, measured, positions))
        peak = jnp.max(probe_field[0] * probe_field[0] + probe_field[1] * probe_field[1])
        object_field = object_field - object_rate / peak * obj_grads
        probe_field = probe_field - probe_rate * lax.optimization_barrier(jnp.sum(probe_grads, 0)) / (jnp.sum(energies) / (size * size))
    proj = object_field
    count = proj.shape[0]
    wave_cos, wave_sin = tables_exact(count, angle_list)
    flat = proj.reshape(count, -1)
    exact = lax.Precision.HIGHEST
    part_cos = jnp.dot(wave_cos, flat, precision=exact, preferred_element_type=jnp.float32).reshape(proj.shape)
    part_sin = jnp.dot(wave_sin, flat, precision=exact, preferred_element_type=jnp.float32).reshape(proj.shape)
    harm_re = part_cos[:, 0] + part_sin[:, 1]
    harm_im = part_cos[:, 1] - part_sin[:, 0]
    harm = jnp.stack([harm_re, harm_im], 1)

    def invert(items):
        block, matrix = items
        return jnp.dot(block.reshape(-1, block.shape[-1]), matrix, precision=exact, preferred_element_type=jnp.float32).reshape(block.shape)
    slices = lax.map(invert, (harm, radial))
    return (slices, probe_field)
```

```python
import functools
import math

import jax
import jax.numpy as jnp
import numpy as np
from jax import lax
from jax.experimental import pallas as pl
from jax.experimental.pallas import tpu as pltpu
from jax.sharding import PartitionSpec as P

ITERS = 2
CHUNKS = 4
LANES = 128
SUBLANES = 8

object_rate = 0.5
probe_rate = 1.0

VMEM_SPEC = pl.BlockSpec(memory_space=pltpu.VMEM)
SMEM_SPEC = pl.BlockSpec(memory_space=pltpu.SMEM)
ANY_SPEC = pl.BlockSpec(memory_space=pl.ANY)


def tables_exact(count, index_list):
    index = jnp.arange(count, dtype=jnp.int32)
    phase = index[:, None] * index_list[None, :] % count
    angle = phase.astype(jnp.float32) * (2.0 * math.pi / count)
    scale = 1.0 / math.sqrt(count)
    return (jnp.cos(angle) * scale, jnp.sin(angle) * scale)


def block_tables(count):
    index = np.arange(count)
    phase = index[:, None] * index[None, :] % count
    angle = phase.astype(np.float32) * np.float32(2.0 * math.pi / count)
    scale = np.float32(1.0 / math.sqrt(count))
    cosine, sine = np.cos(angle) * scale, np.sin(angle) * scale
    forward = np.block([[cosine, sine], [-sine, cosine]]).astype(jnp.bfloat16)
    inverse = np.block([[cosine, -sine], [sine, cosine]]).astype(jnp.bfloat16)
    return forward, inverse


def dot32(a, b):
    return jnp.dot(a, b, preferred_element_type=jnp.float32)


def gradient_kernel(
    pos_ref, obj_ref, meas_ref, prb_ref, fwd_ref, inv_ref,
    out_ref, pg_ref, en_ref,
    pad, piece, wave, mid, acc,
):
    patches, size = meas_ref.shape[0], meas_ref.shape[1]
    cols = obj_ref.shape[2]
    pad[:, :, :cols] = obj_ref[...]
    pad[:, :, cols:] = jnp.zeros((2, size, size), jnp.float32)
    acc[...] = jnp.zeros_like(acc)
    lane = lax.broadcasted_iota(jnp.int32, (size, size), 1)
    probe_re, probe_im = prb_ref[0], prb_ref[1]
    pairs = [(n, min(2, patches - n)) for n in range(0, patches, 2)]

    def place(n):
        col = pos_ref[n, 1]
        base = col // size
        return pl.multiple_of(base * size, size), col - base * size

    energy = jnp.zeros((SUBLANES, size), jnp.float32)
    for n in range(patches):
        start, off = place(n)
        back = lax.rem(size - off, size)
        keep = lane < size - off
        parts = []
        for c in range(2):
            left = pltpu.roll(pad[c, :, pl.ds(start, size)], back, 1)
            right = pltpu.roll(pad[c, :, pl.ds(start + size, size)], back, 1)
            parts.append(jnp.where(keep, left, right))
        p_re, p_im = parts
        piece[n, 0] = p_re
        piece[n, 1] = p_im
        energy += jnp.sum((p_re * p_re + p_im * p_im).reshape(-1, SUBLANES, size), 0)
        wave[:size, n * size:(n + 1) * size] = (probe_re * p_re - probe_im * p_im).astype(jnp.bfloat16)
        wave[size:, n * size:(n + 1) * size] = (probe_re * p_im + probe_im * p_re).astype(jnp.bfloat16)
    en_ref[...] = energy

    def left_product(table_ref):
        for n, many in pairs:
            got = dot32(table_ref[...], wave[:, n * size:(n + many) * size]).astype(jnp.bfloat16)
            for i in range(many):
                rows = slice((n + i) * size, (n + i + 1) * size)
                mid[rows, :size] = got[:size, i * size:(i + 1) * size]
                mid[rows, size:] = got[size:, i * size:(i + 1) * size]

    left_product(fwd_ref)
    for n in range(patches):
        far = dot32(mid[n * size:(n + 1) * size, :], inv_ref[...])
        far_re, far_im = far[:, :size], far[:, size:]
        resid = far_re * far_re + far_im * far_im - meas_ref[n].astype(jnp.float32)
        wave[:size, n * size:(n + 1) * size] = (resid * far_re).astype(jnp.bfloat16)
        wave[size:, n * size:(n + 1) * size] = (resid * far_im).astype(jnp.bfloat16)
    left_product(inv_ref)
    for n in range(patches):
        start, off = place(n)
        grad = dot32(mid[n * size:(n + 1) * size, :], fwd_ref[...])
        g_re, g_im = grad[:, :size], grad[:, size:]
        p_re, p_im = piece[n, 0], piece[n, 1]
        pg_re = p_re * g_re + p_im * g_im
        pg_im = p_re * g_im - p_im * g_re
        if n == 0:
            pg_ref[0], pg_ref[1] = pg_re, pg_im
        else:
            pg_ref[0] += pg_re
            pg_ref[1] += pg_im
        steps = (probe_re * g_re + probe_im * g_im, probe_re * g_im - probe_im * g_re)
        for c in range(2):
            turned = pltpu.roll(steps[c], lax.rem(off, size), 1)
            acc[c, :, pl.ds(start, size)] += jnp.where(lane >= off, turned, 0.0)
            acc[c, :, pl.ds(start + size, size)] += jnp.where(lane < off, turned, 0.0)
    peak = jnp.max(probe_re * probe_re + probe_im * probe_im)
    out_ref[...] = obj_ref[...] - object_rate / peak * acc[:, :, :cols]


def gradient_call(obj, measured, positions, probe, forward, inverse):
    patches, size = measured.shape[0], measured.shape[1]
    rows, cols = obj.shape[1:]
    f32 = jnp.float32
    return pl.pallas_call(
        gradient_kernel,
        name="gradient",
        out_shape=(
            jax.ShapeDtypeStruct(obj.shape, f32),
            jax.ShapeDtypeStruct(probe.shape, f32),
            jax.ShapeDtypeStruct((SUBLANES, size), f32),
        ),
        in_specs=[SMEM_SPEC] + [VMEM_SPEC] * 5,
        out_specs=(VMEM_SPEC,) * 3,
        scratch_shapes=[
            pltpu.VMEM((2, rows, cols + size), f32),
            pltpu.VMEM((patches, 2, size, size), f32),
            pltpu.VMEM((2 * size, patches * size), jnp.bfloat16),
            pltpu.VMEM((patches * size, 2 * size), jnp.bfloat16),
            pltpu.VMEM((2, rows, cols + size), f32),
        ],
        compiler_params=pltpu.CompilerParams(vmem_limit_bytes=40 * 1024 * 1024),
        cost_estimate=pl.CostEstimate(
            flops=patches * 4 * 2 * 4 * size**3, bytes_accessed=4 * 2**20, transcendentals=0
        ),
    )(positions, obj, measured, probe, forward, inverse)


def enter(n, me):
    barrier = pltpu.get_barrier_semaphore()

    def greet(i, carry):
        pl.semaphore_signal(
            barrier, inc=1, device_id={"angle": lax.rem(me + i, n)},
            device_id_type=pl.DeviceIdType.MESH,
        )
        return carry

    lax.fori_loop(1, n, greet, 0)
    pl.semaphore_wait(barrier, n - 1)


def send(n, me, make):
    def one(i, carry):
        d = lax.rem(me + i, n)
        src, dst, send_sem, recv_sem = make(d)
        pltpu.make_async_remote_copy(
            src_ref=src, dst_ref=dst, send_sem=send_sem, recv_sem=recv_sem,
            device_id={"angle": d}, device_id_type=pl.DeviceIdType.MESH,
        ).start()
        return carry

    lax.fori_loop(1, n, one, 0)


def drain(ref, sem):
    pltpu.make_async_copy(ref, ref, sem).wait()


def rows_at(d, count):
    return pl.ds(pl.multiple_of(d * count, SUBLANES), count)


class Reduction:
    def __init__(self, n, me, pg_ref, en_ref, prb_ref, got_pg, got_en, full, sems):
        self.n, self.me = n, me
        self.pg_ref, self.en_ref, self.prb_ref = pg_ref, en_ref, prb_ref
        self.got_pg, self.got_en, self.full, self.sems = got_pg, got_en, full, sems
        self.share = pg_ref.shape[0] // n

    @staticmethod
    def scratch(n, rows, size):
        return [
            pltpu.VMEM((n, rows // n, size), jnp.float32),
            pltpu.VMEM((n, SUBLANES, size), jnp.float32),
            pltpu.VMEM((rows, size), jnp.float32),
            pltpu.SemaphoreType.DMA((6,)),
        ]

    def scatter(self):
        n, me, sems = self.n, self.me, self.sems
        send(n, me, lambda d: (self.pg_ref.at[rows_at(d, self.share)], self.got_pg.at[me], sems.at[0], sems.at[1]))
        send(n, me, lambda d: (self.en_ref, self.got_en.at[me], sems.at[2], sems.at[3]))
        self.got_pg[me] = self.pg_ref[rows_at(me, self.share), :]
        self.got_en[me] = self.en_ref[...]

    def gather(self):
        n, me, sems = self.n, self.me, self.sems
        drain(self.got_pg.at[pl.ds(0, n - 1)], sems.at[1])
        drain(self.got_en.at[pl.ds(0, n - 1)], sems.at[3])
        size = self.prb_ref.shape[1]
        total = jnp.sum(self.got_pg[...], 0)
        energy = jnp.sum(self.got_en[...])
        mine = rows_at(me, self.share)
        self.full[mine, :] = self.prb_ref[mine, :] - probe_rate * total / (energy / (size * size))
        send(n, me, lambda d: (self.full.at[mine], self.full.at[mine], sems.at[4], sems.at[5]))

    def finish(self, out_ref):
        sems, n = self.sems, self.n
        rest = self.full.at[pl.ds(0, (n - 1) * self.share)]
        drain(rest, sems.at[5])
        out_ref[...] = self.full[...]
        drain(self.got_pg.at[pl.ds(0, n - 1)], sems.at[0])
        drain(self.got_en.at[pl.ds(0, n - 1)], sems.at[2])
        drain(rest, sems.at[4])


def reduce_kernel(n, pg_ref, en_ref, prb_ref, out_ref, got_pg, got_en, full, sems):
    me = lax.axis_index("angle")
    red = Reduction(n, me, pg_ref, en_ref, prb_ref, got_pg, got_en, full, sems)
    enter(n, me)
    red.scatter()
    red.gather()
    red.finish(out_ref)


def reduce_call(n, grad, energy, probe):
    rows, size = probe.shape[0] * probe.shape[1], probe.shape[2]
    return pl.pallas_call(
        functools.partial(reduce_kernel, n),
        name="probe_reduce",
        out_shape=jax.ShapeDtypeStruct((rows, size), jnp.float32),
        in_specs=[VMEM_SPEC] * 3,
        out_specs=VMEM_SPEC,
        scratch_shapes=Reduction.scratch(n, rows, size),
        compiler_params=pltpu.CompilerParams(collective_id=0, has_side_effects=True),
    )(grad.reshape(rows, size), energy, probe.reshape(rows, size)).reshape(probe.shape)


def invert_kernel(
    n, obj_ref, wc_ref, ws_ref, radial_ref, pg_ref, en_ref, prb_ref,
    out_ref, probe_ref,
    got, spread, harm, matrix, radial_sem, send_a, recv_a, send_b, recv_b,
    got_pg, got_en, full, sems,
):
    me = lax.axis_index("angle")
    rows, cols = obj_ref.shape[1:]
    share, wide = rows // n, cols // CHUNKS
    load = pltpu.make_async_copy(radial_ref, matrix, radial_sem)
    load.start()
    red = Reduction(n, me, pg_ref, en_ref, prb_ref, got_pg, got_en, full, sems)
    enter(n, me)
    red.scatter()
    spans = [pl.ds(q * wide, wide) for q in range(CHUNKS)]
    for q, span in enumerate(spans):
        send(n, me, lambda d: (
            obj_ref.at[:, rows_at(d, share), span], got.at[me, :, :, span], send_a.at[q], recv_a.at[q]
        ))
    got[me] = obj_ref[:, rows_at(me, share), :]
    red.gather()
    for q, span in enumerate(spans):
        drain(got.at[pl.ds(0, n - 1), :, :, span], recv_a.at[q])

        def harmonic(k, carry):
            re = jnp.zeros((share, wide), jnp.float32)
            im = jnp.zeros((share, wide), jnp.float32)
            for b in range(n):
                wc, ws = wc_ref[k, b], ws_ref[k, b]
                pr, pi = got[b, 0, :, span], got[b, 1, :, span]
                re += wc * pr + ws * pi
                im += wc * pi - ws * pr
            spread[k, 0, :, span] = re
            spread[k, 1, :, span] = im
            return carry

        lax.fori_loop(0, n, harmonic, 0)
        send(n, me, lambda d: (
            spread.at[d, :, :, span], harm.at[:, rows_at(me, share), span], send_b.at[q], recv_b.at[q]
        ))
        harm[:, rows_at(me, share), span] = spread[me, :, :, span]
    load.wait()
    for q, span in enumerate(spans):
        drain(harm.at[:, pl.ds(0, (n - 1) * share), span], recv_b.at[q])
        part = jnp.dot(
            harm[:, :, span].reshape(2 * rows, wide), matrix[span, :],
            precision=lax.Precision.HIGHEST, preferred_element_type=jnp.float32,
        )
        if q == 0:
            out_ref[...] = part
        else:
            out_ref[...] += part
    red.finish(probe_ref)
    for q, span in enumerate(spans):
        drain(got.at[pl.ds(0, n - 1), :, :, span], send_a.at[q])
        drain(got.at[pl.ds(0, n - 1), :, :, span], send_b.at[q])


def invert_call(n, obj, wave_cos, wave_sin, radial, grad, energy, probe):
    rows, cols = obj.shape[1:]
    prows, size = probe.shape[0] * probe.shape[1], probe.shape[2]
    f32 = jnp.float32
    slices, probe_out = pl.pallas_call(
        functools.partial(invert_kernel, n),
        name="invert",
        out_shape=(
            jax.ShapeDtypeStruct((2 * rows, cols), f32),
            jax.ShapeDtypeStruct((prows, size), f32),
        ),
        in_specs=[VMEM_SPEC, SMEM_SPEC, SMEM_SPEC, ANY_SPEC] + [VMEM_SPEC] * 3,
        out_specs=(VMEM_SPEC,) * 2,
        scratch_shapes=[
            pltpu.VMEM((n, 2, rows // n, cols), f32),
            pltpu.VMEM((n, 2, rows // n, cols), f32),
            pltpu.VMEM((2, rows, cols), f32),
            pltpu.VMEM((cols, cols), f32),
            pltpu.SemaphoreType.DMA,
        ]
        + [pltpu.SemaphoreType.DMA((CHUNKS,))] * 4
        + Reduction.scratch(n, prows, size),
        compiler_params=pltpu.CompilerParams(
            collective_id=1, has_side_effects=True, vmem_limit_bytes=40 * 1024 * 1024
        ),
    )(obj, wave_cos, wave_sin, radial, grad.reshape(prows, size), energy, probe.reshape(prows, size))
    return slices.reshape(obj.shape), probe_out.reshape(probe.shape)


def angular(block, wave_cos, wave_sin):
    count = block.shape[0]
    flat = block.reshape(count, -1)
    exact = lax.Precision.HIGHEST
    part_cos = jnp.dot(wave_cos, flat, precision=exact, preferred_element_type=jnp.float32).reshape(
        block.shape
    )
    part_sin = jnp.dot(wave_sin, flat, precision=exact, preferred_element_type=jnp.float32).reshape(
        block.shape
    )
    harm_re = part_cos[:, 0] + part_sin[:, 1]
    harm_im = part_cos[:, 1] - part_sin[:, 0]
    return jnp.stack([harm_re, harm_im], 1)


def probe_step(probe, grad, energy):
    size = probe.shape[1]
    total, energy_total = lax.psum((grad, jnp.sum(energy)), "angle")
    return probe - probe_rate * total / (energy_total / (size * size))


def invert_plain(obj, wave_cos, wave_sin, radial):
    gathered = lax.all_to_all(obj, "angle", split_axis=2, concat_axis=0, tiled=True)
    harm = lax.all_to_all(
        angular(gathered, wave_cos, wave_sin), "angle", split_axis=0, concat_axis=2, tiled=True
    )
    return jnp.einsum(
        "kcrn,knm->kcrm",
        harm,
        radial,
        precision=lax.Precision.HIGHEST,
        preferred_element_type=jnp.float32,
    )


def on_device(n, object_init, measured, positions, angle_list, probe, radial):
    rows, cols = object_init.shape[2:]
    size = probe.shape[1]
    assert object_init.shape[0] == 1 and radial.shape[0] == 1
    assert rows == size and size == LANES and cols % (LANES * CHUNKS) == 0
    direct = rows % (n * SUBLANES) == 0
    forward, inverse = (jnp.asarray(t) for t in block_tables(size))
    wave_cos, wave_sin = tables_exact(angle_list.shape[0], angle_list)
    obj = object_init[0]
    for step in range(ITERS):
        obj, grad, energy = gradient_call(obj, measured[0], positions[0], probe, forward, inverse)
        if not direct:
            probe = probe_step(probe, grad, energy)
        elif step < ITERS - 1:
            probe = reduce_call(n, grad, energy, probe)
    if direct:
        slices, probe = invert_call(n, obj, wave_cos, wave_sin, radial[0], grad, energy, probe)
        return slices[None], probe
    return invert_plain(obj[None], wave_cos, wave_sin, radial), probe


def solution(mesh):
    in_specs = (
        P(("scan", "angle"), None, None, None),
        P(("scan", "angle"), None, None, None),
        P(("scan", "angle"), None, None),
        P("scan"),
        P("scan", None, None),
        P("angle", None, None),
    )
    out_specs = (P(("scan", "angle"), None, None, None), P("scan", None, None))
    return jax.shard_map(
        functools.partial(on_device, mesh.shape["angle"]),
        mesh=mesh, in_specs=in_specs, out_specs=out_specs, check_vma=False,
    )
```

```python
import functools
import math

import jax
import jax.numpy as jnp
import numpy as np
from jax import lax
from jax.experimental import pallas as pl
from jax.experimental.pallas import tpu as pltpu
from jax.sharding import PartitionSpec as P

ITERS = 2
CHUNKS = 4
LANES = 128
SUBLANES = 8

object_rate = 0.5
probe_rate = 1.0

VMEM_SPEC = pl.BlockSpec(memory_space=pltpu.VMEM)
SMEM_SPEC = pl.BlockSpec(memory_space=pltpu.SMEM)
ANY_SPEC = pl.BlockSpec(memory_space=pl.ANY)


def tables_exact(count, index_list):
    index = jnp.arange(count, dtype=jnp.int32)
    phase = index[:, None] * index_list[None, :] % count
    angle = phase.astype(jnp.float32) * (2.0 * math.pi / count)
    scale = 1.0 / math.sqrt(count)
    return (jnp.cos(angle) * scale, jnp.sin(angle) * scale)


def block_tables(count):
    index = np.arange(count)
    phase = index[:, None] * index[None, :] % count
    angle = phase.astype(np.float32) * np.float32(2.0 * math.pi / count)
    scale = np.float32(1.0 / math.sqrt(count))
    cosine, sine = np.cos(angle) * scale, np.sin(angle) * scale
    forward = np.block([[cosine, sine], [-sine, cosine]]).astype(jnp.bfloat16)
    inverse = np.block([[cosine, -sine], [sine, cosine]]).astype(jnp.bfloat16)
    return forward, inverse


def dot32(a, b):
    return jnp.dot(a, b, preferred_element_type=jnp.float32)


def greet(n, me):
    barrier = pltpu.get_barrier_semaphore()

    def one(i, carry):
        pl.semaphore_signal(
            barrier, inc=1, device_id={"angle": lax.rem(me + i, n)},
            device_id_type=pl.DeviceIdType.MESH,
        )
        return carry

    lax.fori_loop(1, n, one, 0)


def send(n, me, make):
    def one(i, carry):
        d = lax.rem(me + i, n)
        src, dst, send_sem, recv_sem = make(d)
        pltpu.make_async_remote_copy(
            src_ref=src, dst_ref=dst, send_sem=send_sem, recv_sem=recv_sem,
            device_id={"angle": d}, device_id_type=pl.DeviceIdType.MESH,
        ).start()
        return carry

    lax.fori_loop(1, n, one, 0)


def drain(ref, sem):
    pltpu.make_async_copy(ref, ref, sem).wait()


def rows_at(d, count):
    return pl.ds(pl.multiple_of(d * count, SUBLANES), count)


def gradient_pass(span, place, obj, meas, probe, fwd_ref, inv_ref, pg, acc, energy, piece, wave, mid, first):
    size = wave.shape[0] // 2
    rows = obj.shape[1]
    tiles = obj.shape[2] // size
    lane = lax.broadcasted_iota(jnp.int32, (rows, size), 1)
    probe_re, probe_im = probe[:size, :], probe[size:, :]
    numbers = range(*span)
    at = {n: i for i, n in enumerate(numbers)}
    tile = lambda ref, c, t: ref[c, :, t * size:(t + 1) * size]

    for n in numbers:
        i = at[n]
        col, turn, low = place(n)
        keep = lane < size - turn
        parts = []
        for c in range(2):
            if 2 * low == n and low > 0:
                before = jnp.full((rows, size), col, jnp.int32) < low * size
                left = jnp.where(before, tile(obj, c, low - 1), tile(obj, c, low))
                right = jnp.where(before, tile(obj, c, low), tile(obj, c, min(low + 1, tiles - 1)))
            else:
                left, right = tile(obj, c, low), tile(obj, c, min(low + 1, tiles - 1))
            back = lax.rem(size - turn, size)
            parts.append(jnp.where(keep, pltpu.roll(left, back, 1), pltpu.roll(right, back, 1)))
        p_re, p_im = parts
        piece[i, 0] = p_re
        piece[i, 1] = p_im
        energy += jnp.sum((p_re * p_re + p_im * p_im).reshape(-1, SUBLANES, size), 0)
        wave[:size, i * size:(i + 1) * size] = (probe_re * p_re - probe_im * p_im).astype(jnp.bfloat16)
        wave[size:, i * size:(i + 1) * size] = (probe_re * p_im + probe_im * p_re).astype(jnp.bfloat16)

    def left_product(table_ref):
        for i in range(0, len(numbers), 2):
            many = min(2, len(numbers) - i)
            got = dot32(table_ref[...], wave[:, i * size:(i + many) * size]).astype(jnp.bfloat16)
            for j in range(many):
                part = slice((i + j) * size, (i + j + 1) * size)
                mid[part, :size] = got[:size, j * size:(j + 1) * size]
                mid[part, size:] = got[size:, j * size:(j + 1) * size]

    left_product(fwd_ref)
    for n in numbers:
        part = slice(at[n] * size, (at[n] + 1) * size)
        far = dot32(mid[part, :], inv_ref[...])
        far_re, far_im = far[:, :size], far[:, size:]
        resid = far_re * far_re + far_im * far_im - meas[n].astype(jnp.float32)
        wave[:size, part] = (resid * far_re).astype(jnp.bfloat16)
        wave[size:, part] = (resid * far_im).astype(jnp.bfloat16)
    left_product(inv_ref)
    for n in numbers:
        i = at[n]
        col, turn, low = place(n)
        grad = dot32(mid[i * size:(i + 1) * size, :], fwd_ref[...])
        g_re, g_im = grad[:, :size], grad[:, size:]
        p_re, p_im = piece[i, 0], piece[i, 1]
        pg_re = p_re * g_re + p_im * g_im
        pg_im = p_re * g_im - p_im * g_re
        if first and i == 0:
            pg[:size, :], pg[size:, :] = pg_re, pg_im
        else:
            pg[:size, :] += pg_re
            pg[size:, :] += pg_im
        steps = (probe_re * g_re + probe_im * g_im, probe_re * g_im - probe_im * g_re)
        ends = [low, low + 1] if 2 * low < n or low == 0 else [low - 1, low, low + 1]
        for c in range(2):
            turned = pltpu.roll(steps[c], turn, 1)
            for t in ends:
                if t < tiles:
                    where = lane + t * size
                    inside = (where >= col) & (where < col + size)
                    acc[c, :, t * size:(t + 1) * size] += jnp.where(inside, turned, 0.0)
    return energy


class Reduction:
    def __init__(self, n, me, pg, en, got_pg, got_en, full, sems):
        self.n, self.me, self.pg, self.en = n, me, pg, en
        self.got_pg, self.got_en, self.full, self.sems = got_pg, got_en, full, sems
        self.share = pg.shape[0] // n

    @staticmethod
    def scratch(n, rows, size):
        return [
            pltpu.VMEM((rows, size), jnp.float32),
            pltpu.VMEM((1, size), jnp.float32),
            pltpu.VMEM((n, rows // n, size), jnp.float32),
            pltpu.VMEM((n, 1, size), jnp.float32),
            pltpu.VMEM((rows, size), jnp.float32),
            pltpu.SemaphoreType.DMA((6,)),
        ]

    def scatter(self):
        n, me, sems = self.n, self.me, self.sems
        send(n, me, lambda d: (self.en, self.got_en.at[me], sems.at[2], sems.at[3]))
        send(n, me, lambda d: (self.pg.at[rows_at(d, self.share)], self.got_pg.at[me], sems.at[0], sems.at[1]))
        self.got_pg[me] = self.pg[rows_at(me, self.share), :]
        self.got_en[me] = self.en[...]

    def gather(self, probe):
        n, me, sems = self.n, self.me, self.sems
        drain(self.got_pg.at[pl.ds(0, n - 1)], sems.at[1])
        drain(self.got_en.at[pl.ds(0, n - 1)], sems.at[3])
        size = probe.shape[1]
        total = jnp.sum(self.got_pg[...], 0)
        energy = jnp.sum(self.got_en[...])
        mine = rows_at(me, self.share)
        self.full[mine, :] = probe[mine, :] - probe_rate * total / (energy / (size * size))
        send(n, me, lambda d: (self.full.at[mine], self.full.at[mine], sems.at[4], sems.at[5]))

    def arrive(self):
        drain(self.full.at[pl.ds(0, (self.n - 1) * self.share)], self.sems.at[5])

    def leave(self):
        sems, n = self.sems, self.n
        drain(self.got_pg.at[pl.ds(0, n - 1)], sems.at[0])
        drain(self.got_en.at[pl.ds(0, n - 1)], sems.at[2])
        drain(self.full.at[pl.ds(0, (n - 1) * self.share)], sems.at[4])


def whole_kernel(
    n, pos_ref, ang_ref, obj_hbm, meas_hbm, prb_hbm, fwd_hbm, inv_hbm, radial_hbm, cos_ref, sin_ref,
    out_ref, probe_ref,
    obj, meas, prb, fwd, inv, acc, piece, wave, mid,
    got, spread, harm, matrix, load_sems, send_a, recv_a, send_b, recv_b, *reds,
):
    me = lax.axis_index("angle")
    rows, cols = obj.shape[1:]
    patches, size = meas.shape[0], meas.shape[1]
    share, wide = rows // n, cols // CHUNKS
    loads = [
        pltpu.make_async_copy(src, dst, load_sems.at[i])
        for i, (src, dst) in enumerate((
            (obj_hbm, obj), (prb_hbm, prb), (fwd_hbm, fwd), (inv_hbm, inv), (meas_hbm, meas), (radial_hbm, matrix),
        ))
    ]
    for load in loads:
        load.start()
    greet(n, me)
    acc[...] = jnp.zeros_like(acc)
    for load in loads[:-1]:
        load.wait()

    def place(k):
        col = pos_ref[0, k, 1]
        return col, lax.rem(col, size), k // 2

    spans = [pl.ds(q * wide, wide) for q in range(CHUNKS)]
    ends = [min(patches, 2 * (wide // size) * (q + 1) + 1) for q in range(CHUNKS)]
    groups = list(zip([0] + ends[:-1], ends))
    each = len(reds) // ITERS
    probe = prb
    for step in range(ITERS):
        red = Reduction(n, me, *reds[step * each:(step + 1) * each])
        pre, pim = probe[:size, :], probe[size:, :]
        rate = object_rate / jnp.max(pre * pre + pim * pim)
        energy = jnp.zeros((SUBLANES, size), jnp.float32)
        for q, group in enumerate(groups):
            energy = gradient_pass(
                group, place, obj, meas, probe, fwd, inv, red.pg, acc, energy, piece, wave, mid, q == 0
            )
            span = spans[q]
            obj[:, :, span] = obj[:, :, span] - rate * acc[:, :, span]
            acc[:, :, span] = jnp.zeros((2, rows, wide), jnp.float32)
            if step == ITERS - 1:
                send(n, me, lambda d: (
                    obj.at[:, rows_at(d, share), span], got.at[me, :, :, span], send_a.at[q], recv_a.at[q]
                ))
        red.en[...] = jnp.sum(energy, 0, keepdims=True)
        if step == 0:
            pl.semaphore_wait(pltpu.get_barrier_semaphore(), n - 1)
        red.scatter()
        if step < ITERS - 1:
            red.gather(probe)
            red.arrive()
            red.leave()
            probe = red.full
    got[me] = obj[:, rows_at(me, share), :]
    red.gather(probe)

    def weight(ref, k, b):
        return ref[lax.rem(k * ang_ref[b], n)]

    for q, span in enumerate(spans):
        drain(got.at[pl.ds(0, n - 1), :, :, span], recv_a.at[q])

        def harmonic(k, carry):
            re = jnp.zeros((share, wide), jnp.float32)
            im = jnp.zeros((share, wide), jnp.float32)
            for b in range(n):
                wc, ws = weight(cos_ref, k, b), weight(sin_ref, k, b)
                pr, pi = got[b, 0, :, span], got[b, 1, :, span]
                re += wc * pr + ws * pi
                im += wc * pi - ws * pr
            spread[k, 0, :, span] = re
            spread[k, 1, :, span] = im
            return carry

        lax.fori_loop(0, n, harmonic, 0)
        send(n, me, lambda d: (
            spread.at[d, :, :, span], harm.at[:, rows_at(me, share), span], send_b.at[q], recv_b.at[q]
        ))
        harm[:, rows_at(me, share), span] = spread[me, :, :, span]
    loads[-1].wait()
    for q, span in enumerate(spans):
        drain(harm.at[:, pl.ds(0, (n - 1) * share), span], recv_b.at[q])
        part = jnp.dot(
            harm[:, :, span].reshape(2 * rows, wide), matrix[span, :],
            precision=lax.Precision.HIGHEST, preferred_element_type=jnp.float32,
        )
        if q == 0:
            out_ref[...] = part
        else:
            out_ref[...] += part
        if q == CHUNKS - 2:
            red.arrive()
            probe_ref[...] = red.full[...]
    red.leave()
    for q, span in enumerate(spans):
        drain(got.at[pl.ds(0, n - 1), :, :, span], send_a.at[q])
        drain(got.at[pl.ds(0, n - 1), :, :, span], send_b.at[q])


def whole_call(n, object_init, measured, positions, angle_list, probe, radial):
    rows, cols = object_init.shape[2:]
    patches, size = measured.shape[1:3]
    prows = 2 * size
    f32, bf16 = jnp.float32, jnp.bfloat16
    forward, inverse = block_tables(size)
    phase = np.arange(n).astype(np.float32) * np.float32(2.0 * math.pi / n)
    scale = np.float32(1.0 / math.sqrt(n))
    slices, probe_out = pl.pallas_call(
        functools.partial(whole_kernel, n),
        name="whole",
        out_shape=(
            jax.ShapeDtypeStruct((2 * rows, cols), f32),
            jax.ShapeDtypeStruct((prows, size), f32),
        ),
        in_specs=[SMEM_SPEC] * 2 + [ANY_SPEC] * 6 + [SMEM_SPEC] * 2,
        out_specs=(VMEM_SPEC,) * 2,
        scratch_shapes=[
            pltpu.VMEM((2, rows, cols), f32),
            pltpu.VMEM((patches, size, size), bf16),
            pltpu.VMEM((prows, size), f32),
            pltpu.VMEM((prows, prows), bf16),
            pltpu.VMEM((prows, prows), bf16),
            pltpu.VMEM((2, rows, cols), f32),
            pltpu.VMEM((patches, 2, size, size), f32),
            pltpu.VMEM((prows, patches * size), bf16),
            pltpu.VMEM((patches * size, prows), bf16),
            pltpu.VMEM((n, 2, rows // n, cols), f32),
            pltpu.VMEM((n, 2, rows // n, cols), f32),
            pltpu.VMEM((2, rows, cols), f32),
            pltpu.VMEM((cols, cols), f32),
            pltpu.SemaphoreType.DMA((6,)),
        ]
        + [pltpu.SemaphoreType.DMA((CHUNKS,))] * 4
        + Reduction.scratch(n, prows, size) * ITERS,
        compiler_params=pltpu.CompilerParams(
            collective_id=0, has_side_effects=True, vmem_limit_bytes=48 * 1024 * 1024
        ),
    )(
        positions, angle_list, object_init.reshape(2, rows, cols), measured.reshape(patches, size, size),
        probe.reshape(prows, size), jnp.asarray(forward), jnp.asarray(inverse), radial.reshape(cols, cols),
        jnp.asarray(np.cos(phase) * scale), jnp.asarray(np.sin(phase) * scale),
    )
    return slices.reshape(object_init.shape), probe_out.reshape(probe.shape)


def tables(count, index_list):
    cosine_part, sine_part = tables_exact(count, index_list)
    return (cosine_part.astype(jnp.bfloat16), sine_part.astype(jnp.bfloat16))


def left(table, field):
    return jnp.einsum("jk,nkl->njl", table, field, preferred_element_type=jnp.float32)


def right(field, table):
    return jnp.einsum("njk,kl->njl", field, table, preferred_element_type=jnp.float32)


def gradient_list(
    object_field, measured_intensity, scan_positions, probe_field, cosine_theta, sine_theta
):
    size = probe_field.shape[1]
    zero_index = jnp.zeros((), jnp.int32)
    pieces = jax.vmap(
        lambda row, col: lax.dynamic_slice(object_field, (zero_index, row, col), (2, size, size))
    )(scan_positions[:, 0], scan_positions[:, 1])
    piece_re, piece_im = (pieces[:, 0], pieces[:, 1])
    probe_re, probe_im = (probe_field[0], probe_field[1])
    wave_re = (probe_re * piece_re - probe_im * piece_im).astype(jnp.bfloat16)
    wave_im = (probe_re * piece_im + probe_im * piece_re).astype(jnp.bfloat16)
    half_re = (left(cosine_theta, wave_re) + left(sine_theta, wave_im)).astype(jnp.bfloat16)
    half_im = (left(cosine_theta, wave_im) - left(sine_theta, wave_re)).astype(jnp.bfloat16)
    farfield_real = right(half_re, cosine_theta) + right(half_im, sine_theta)
    farfield_imaginary = right(half_im, cosine_theta) - right(half_re, sine_theta)
    residual_error = (
        farfield_real * farfield_real
        + farfield_imaginary * farfield_imaginary
        - measured_intensity.astype(jnp.float32)
    )
    push_re = (residual_error * farfield_real).astype(jnp.bfloat16)
    push_im = (residual_error * farfield_imaginary).astype(jnp.bfloat16)
    back_re = (left(cosine_theta, push_re) - left(sine_theta, push_im)).astype(jnp.bfloat16)
    back_im = (left(cosine_theta, push_im) + left(sine_theta, push_re)).astype(jnp.bfloat16)
    grad_re = right(back_re, cosine_theta) - right(back_im, sine_theta)
    grad_im = right(back_im, cosine_theta) + right(back_re, sine_theta)
    step_re = probe_re * grad_re + probe_im * grad_im
    step_im = probe_re * grad_im - probe_im * grad_re
    steps_all = jnp.stack([step_re, step_im], 1)

    def place(index, total):
        start = (zero_index, scan_positions[index, 0], scan_positions[index, 1])
        current = lax.dynamic_slice(total, start, (2, size, size))
        return lax.dynamic_update_slice(total, current + steps_all[index], start)

    obj_grad = lax.fori_loop(0, scan_positions.shape[0], place, jnp.zeros_like(object_field))
    pg_re = jnp.sum(piece_re * grad_re + piece_im * grad_im, 0)
    pg_im = jnp.sum(piece_re * grad_im - piece_im * grad_re, 0)
    energy = jnp.sum(piece_re * piece_re + piece_im * piece_im)
    return (obj_grad, jnp.stack([pg_re, pg_im], 0), energy)


def angular(block, wave_cos, wave_sin):
    count = block.shape[0]
    flat = block.reshape(count, -1)
    exact = lax.Precision.HIGHEST
    part_cos = jnp.dot(wave_cos, flat, precision=exact, preferred_element_type=jnp.float32).reshape(
        block.shape
    )
    part_sin = jnp.dot(wave_sin, flat, precision=exact, preferred_element_type=jnp.float32).reshape(
        block.shape
    )
    harm_re = part_cos[:, 0] + part_sin[:, 1]
    harm_im = part_cos[:, 1] - part_sin[:, 0]
    return jnp.stack([harm_re, harm_im], 1)


def plain_device(object_init, measured, positions, angle_list, probe, radial):
    size = probe.shape[1]
    cosine_theta, sine_theta = tables(size, jnp.arange(size, dtype=jnp.int32))
    object_field = object_init
    probe_field = probe
    for step in range(ITERS):

        def one(items):
            return gradient_list(
                items[0], items[1], items[2], probe_field, cosine_theta, sine_theta
            )

        obj_grads, probe_grads, energies = lax.map(one, (object_field, measured, positions))
        probe_total, energy_total = lax.psum((jnp.sum(probe_grads, 0), jnp.sum(energies)), "angle")
        peak = jnp.max(probe_field[0] * probe_field[0] + probe_field[1] * probe_field[1])
        object_field = object_field - object_rate / peak * obj_grads
        probe_field = probe_field - probe_rate * probe_total / (energy_total / (size * size))
    wave_cos, wave_sin = tables_exact(angle_list.shape[0], angle_list)
    gathered = lax.all_to_all(object_field, "angle", split_axis=2, concat_axis=0, tiled=True)
    harm = lax.all_to_all(
        angular(gathered, wave_cos, wave_sin), "angle", split_axis=0, concat_axis=2, tiled=True
    )
    slices = jnp.einsum(
        "kcrn,knm->kcrm",
        harm,
        radial,
        precision=lax.Precision.HIGHEST,
        preferred_element_type=jnp.float32,
    )
    return (slices, probe_field)


def on_device(n, object_init, measured, positions, angle_list, probe, radial):
    rows, cols = object_init.shape[2:]
    patches, size = measured.shape[1:3]
    fits = (
        object_init.shape[0] == 1
        and radial.shape[0] == 1
        and angle_list.shape[0] == n
        and rows == size == LANES
        and cols % (LANES * CHUNKS) == 0
        and patches == 2 * cols // size - 1
        and rows % (n * SUBLANES) == 0
    )
    device = functools.partial(whole_call, n) if fits else plain_device
    return device(object_init, measured, positions, angle_list, probe, radial)


def solution(mesh):
    in_specs = (
        P(("scan", "angle"), None, None, None),
        P(("scan", "angle"), None, None, None),
        P(("scan", "angle"), None, None),
        P("scan"),
        P("scan", None, None),
        P("angle", None, None),
    )
    out_specs = (P(("scan", "angle"), None, None, None), P("scan", None, None))
    return jax.shard_map(
        functools.partial(on_device, mesh.shape["angle"]),
        mesh=mesh, in_specs=in_specs, out_specs=out_specs, check_vma=False,
    )
```

```python
import functools
import math

import jax
import jax.numpy as jnp
import numpy as np
from jax import lax
from jax.experimental import pallas as pl
from jax.experimental.pallas import tpu as pltpu
from jax.sharding import PartitionSpec as P

ITERS = 2
CHUNKS = 4
GROUP = 4
LANES = 128
SUBLANES = 8

object_rate = 0.5
probe_rate = 1.0

VMEM_SPEC = pl.BlockSpec(memory_space=pltpu.VMEM)
SMEM_SPEC = pl.BlockSpec(memory_space=pltpu.SMEM)
HBM_SPEC = pl.BlockSpec(memory_space=pltpu.HBM)


def tables_exact(count, index_list):
    index = jnp.arange(count, dtype=jnp.int32)
    phase = index[:, None] * index_list[None, :] % count
    angle = phase.astype(jnp.float32) * (2.0 * math.pi / count)
    scale = 1.0 / math.sqrt(count)
    return (jnp.cos(angle) * scale, jnp.sin(angle) * scale)


def block_tables(count):
    index = np.arange(count)
    phase = index[:, None] * index[None, :] % count
    angle = phase.astype(np.float32) * np.float32(2.0 * math.pi / count)
    scale = np.float32(1.0 / math.sqrt(count))
    cosine, sine = np.cos(angle) * scale, np.sin(angle) * scale
    forward = np.block([[cosine, sine], [-sine, cosine]]).astype(jnp.bfloat16)
    inverse = np.block([[cosine, -sine], [sine, cosine]]).astype(jnp.bfloat16)
    return forward, inverse


def dot32(a, b):
    return jnp.dot(a, b, preferred_element_type=jnp.float32)


def greet(n, me):
    barrier = pltpu.get_barrier_semaphore()

    def one(i, carry):
        pl.semaphore_signal(
            barrier, inc=1, device_id={"angle": lax.rem(me + i, n)},
            device_id_type=pl.DeviceIdType.MESH,
        )
        return carry

    lax.fori_loop(1, n, one, 0)


def send(n, me, make):
    def one(i, carry):
        d = lax.rem(me + i, n)
        src, dst, send_sem, recv_sem = make(d)
        pltpu.make_async_remote_copy(
            src_ref=src, dst_ref=dst, send_sem=send_sem, recv_sem=recv_sem,
            device_id={"angle": d}, device_id_type=pl.DeviceIdType.MESH,
        ).start()
        return carry

    lax.fori_loop(1, n, one, 0)


def send_along(count, mine, peer, make):
    def one(i, carry):
        j = lax.rem(mine + i, count)
        src, dst, send_sem, recv_sem = make(j)
        pltpu.make_async_remote_copy(
            src_ref=src, dst_ref=dst, send_sem=send_sem, recv_sem=recv_sem,
            device_id={"angle": peer(j)}, device_id_type=pl.DeviceIdType.MESH,
        ).start()
        return carry

    lax.fori_loop(1, count, one, 0)


def drain(ref, sem):
    pltpu.make_async_copy(ref, ref, sem).wait()


def rows_at(d, count):
    return pl.ds(pl.multiple_of(d * count, SUBLANES), count)


def gradient_pass(span, place, obj, meas, probe, fwd_ref, inv_ref, pg, acc, energy, piece, wave, mid, first):
    size = wave.shape[0] // 2
    rows = obj.shape[1]
    tiles = obj.shape[2] // size
    lane = lax.broadcasted_iota(jnp.int32, (rows, size), 1)
    probe_re, probe_im = probe[:size, :], probe[size:, :]
    numbers = range(*span)
    at = {n: i for i, n in enumerate(numbers)}
    tile = lambda ref, c, t: ref[c, :, t * size:(t + 1) * size]

    for n in numbers:
        i = at[n]
        col, turn, low = place(n)
        keep = lane < size - turn
        parts = []
        for c in range(2):
            if 2 * low == n and low > 0:
                before = jnp.full((rows, size), col, jnp.int32) < low * size
                left = jnp.where(before, tile(obj, c, low - 1), tile(obj, c, low))
                right = jnp.where(before, tile(obj, c, low), tile(obj, c, min(low + 1, tiles - 1)))
            else:
                left, right = tile(obj, c, low), tile(obj, c, min(low + 1, tiles - 1))
            back = lax.rem(size - turn, size)
            parts.append(jnp.where(keep, pltpu.roll(left, back, 1), pltpu.roll(right, back, 1)))
        p_re, p_im = parts
        piece[i, 0] = p_re
        piece[i, 1] = p_im
        energy += jnp.sum((p_re * p_re + p_im * p_im).reshape(-1, SUBLANES, size), 0)
        wave[:size, i * size:(i + 1) * size] = (probe_re * p_re - probe_im * p_im).astype(jnp.bfloat16)
        wave[size:, i * size:(i + 1) * size] = (probe_re * p_im + probe_im * p_re).astype(jnp.bfloat16)

    def left_product(table_ref):
        for i in range(0, len(numbers), 2):
            many = min(2, len(numbers) - i)
            got = dot32(table_ref[...], wave[:, i * size:(i + many) * size]).astype(jnp.bfloat16)
            for j in range(many):
                part = slice((i + j) * size, (i + j + 1) * size)
                mid[part, :size] = got[:size, j * size:(j + 1) * size]
                mid[part, size:] = got[size:, j * size:(j + 1) * size]

    left_product(fwd_ref)
    for n in numbers:
        part = slice(at[n] * size, (at[n] + 1) * size)
        far = dot32(mid[part, :], inv_ref[...])
        far_re, far_im = far[:, :size], far[:, size:]
        resid = far_re * far_re + far_im * far_im - meas[n].astype(jnp.float32)
        wave[:size, part] = (resid * far_re).astype(jnp.bfloat16)
        wave[size:, part] = (resid * far_im).astype(jnp.bfloat16)
    left_product(inv_ref)
    for n in numbers:
        i = at[n]
        col, turn, low = place(n)
        grad = dot32(mid[i * size:(i + 1) * size, :], fwd_ref[...])
        g_re, g_im = grad[:, :size], grad[:, size:]
        p_re, p_im = piece[i, 0], piece[i, 1]
        pg_re = p_re * g_re + p_im * g_im
        pg_im = p_re * g_im - p_im * g_re
        if first and i == 0:
            pg[:size, :], pg[size:, :] = pg_re, pg_im
        else:
            pg[:size, :] += pg_re
            pg[size:, :] += pg_im
        steps = (probe_re * g_re + probe_im * g_im, probe_re * g_im - probe_im * g_re)
        ends = [low, low + 1] if 2 * low < n or low == 0 else [low - 1, low, low + 1]
        for c in range(2):
            turned = pltpu.roll(steps[c], turn, 1)
            for t in ends:
                if t < tiles:
                    where = lane + t * size
                    inside = (where >= col) & (where < col + size)
                    acc[c, :, t * size:(t + 1) * size] += jnp.where(inside, turned, 0.0)
    return energy


class Reduction:
    def __init__(self, n, me, pg, en, got_pg, got_en, full, sems):
        self.n, self.me, self.pg, self.en = n, me, pg, en
        self.got_pg, self.got_en, self.full, self.sems = got_pg, got_en, full, sems
        self.share = pg.shape[0] // n

    @staticmethod
    def scratch(n, rows, size):
        return [
            pltpu.VMEM((rows, size), jnp.float32),
            pltpu.VMEM((1, size), jnp.float32),
            pltpu.VMEM((n, rows // n, size), jnp.float32),
            pltpu.VMEM((n, 1, size), jnp.float32),
            pltpu.VMEM((rows, size), jnp.float32),
            pltpu.SemaphoreType.DMA((6,)),
        ]

    def scatter(self):
        n, me, sems = self.n, self.me, self.sems
        send(n, me, lambda d: (self.en, self.got_en.at[me], sems.at[2], sems.at[3]))
        send(n, me, lambda d: (self.pg.at[rows_at(d, self.share)], self.got_pg.at[me], sems.at[0], sems.at[1]))
        self.got_pg[me] = self.pg[rows_at(me, self.share), :]
        self.got_en[me] = self.en[...]

    def gather(self, probe):
        n, me, sems = self.n, self.me, self.sems
        drain(self.got_pg.at[pl.ds(0, n - 1)], sems.at[1])
        drain(self.got_en.at[pl.ds(0, n - 1)], sems.at[3])
        size = probe.shape[1]
        total = jnp.sum(self.got_pg[...], 0)
        energy = jnp.sum(self.got_en[...])
        mine = rows_at(me, self.share)
        self.full[mine, :] = probe[mine, :] - probe_rate * total / (energy / (size * size))
        send(n, me, lambda d: (self.full.at[mine], self.full.at[mine], sems.at[4], sems.at[5]))

    def arrive(self):
        drain(self.full.at[pl.ds(0, (self.n - 1) * self.share)], self.sems.at[5])

    def leave(self):
        sems, n = self.sems, self.n
        drain(self.got_pg.at[pl.ds(0, n - 1)], sems.at[0])
        drain(self.got_en.at[pl.ds(0, n - 1)], sems.at[2])
        drain(self.full.at[pl.ds(0, (n - 1) * self.share)], sems.at[4])


class Nested:
    def __init__(self, n, me, pg, en, got_a, en_a, part, en_part, got_b, en_b, full, sems):
        self.g, self.m = GROUP, n // GROUP
        self.u, self.z = lax.rem(me, GROUP), me // GROUP
        self.pg, self.en, self.full, self.sems = pg, en, full, sems
        self.got_a, self.en_a, self.part, self.en_part = got_a, en_a, part, en_part
        self.got_b, self.en_b = got_b, en_b
        self.coarse, self.fine = pg.shape[0] // GROUP, pg.shape[0] // n

    @staticmethod
    def scratch(n, rows, size):
        f32, m = jnp.float32, n // GROUP
        return [
            pltpu.VMEM((rows, size), f32),
            pltpu.VMEM((1, size), f32),
            pltpu.VMEM((GROUP, rows // GROUP, size), f32),
            pltpu.VMEM((GROUP, 1, size), f32),
            pltpu.VMEM((rows // GROUP, size), f32),
            pltpu.VMEM((1, size), f32),
            pltpu.VMEM((m, rows // n, size), f32),
            pltpu.VMEM((m, 1, size), f32),
            pltpu.VMEM((rows, size), f32),
            pltpu.SemaphoreType.DMA((12,)),
        ]

    def near(self, j):
        return self.z * self.g + j

    def across(self, j):
        return j * self.g + self.u

    def mine(self):
        return pl.ds(pl.multiple_of(self.u * self.coarse + self.z * self.fine, SUBLANES), self.fine)

    def scatter(self):
        g, u, sems = self.g, self.u, self.sems
        send_along(g, u, self.near, lambda j: (
            self.pg.at[rows_at(j, self.coarse)], self.got_a.at[u], sems.at[0], sems.at[1]
        ))
        send_along(g, u, self.near, lambda j: (self.en, self.en_a.at[u], sems.at[2], sems.at[3]))
        self.got_a[u] = self.pg[rows_at(u, self.coarse), :]
        self.en_a[u] = self.en[...]

    def cross(self):
        g, m, z, sems = self.g, self.m, self.z, self.sems
        drain(self.got_a.at[pl.ds(0, g - 1)], sems.at[1])
        drain(self.en_a.at[pl.ds(0, g - 1)], sems.at[3])
        self.part[...] = jnp.sum(self.got_a[...], 0)
        self.en_part[...] = jnp.sum(self.en_a[...], 0)
        send_along(m, z, self.across, lambda j: (
            self.part.at[rows_at(j, self.fine)], self.got_b.at[z], sems.at[4], sems.at[5]
        ))
        send_along(m, z, self.across, lambda j: (self.en_part, self.en_b.at[z], sems.at[6], sems.at[7]))
        self.got_b[z] = self.part[rows_at(z, self.fine), :]
        self.en_b[z] = self.en_part[...]

    def gather(self, probe):
        m, z, sems, mine = self.m, self.z, self.sems, self.mine()
        drain(self.got_b.at[pl.ds(0, m - 1)], sems.at[5])
        drain(self.en_b.at[pl.ds(0, m - 1)], sems.at[7])
        size = probe.shape[1]
        total = jnp.sum(self.got_b[...], 0)
        energy = jnp.sum(self.en_b[...])
        self.full[mine, :] = probe[mine, :] - probe_rate * total / (energy / (size * size))
        send_along(m, z, self.across, lambda j: (
            self.full.at[mine], self.full.at[mine], sems.at[8], sems.at[9]
        ))

    def share(self):
        g, m, u, sems = self.g, self.m, self.u, self.sems
        drain(self.full.at[pl.ds(0, (m - 1) * self.fine)], sems.at[9])
        rows = rows_at(u, self.coarse)
        send_along(g, u, self.near, lambda j: (
            self.full.at[rows], self.full.at[rows], sems.at[10], sems.at[11]
        ))

    def arrive(self):
        drain(self.full.at[pl.ds(0, (self.g - 1) * self.coarse)], self.sems.at[11])

    def leave(self):
        g, m, sems = self.g, self.m, self.sems
        drain(self.got_a.at[pl.ds(0, g - 1)], sems.at[0])
        drain(self.en_a.at[pl.ds(0, g - 1)], sems.at[2])
        drain(self.got_b.at[pl.ds(0, m - 1)], sems.at[4])
        drain(self.en_b.at[pl.ds(0, m - 1)], sems.at[6])
        drain(self.full.at[pl.ds(0, (m - 1) * self.fine)], sems.at[8])
        drain(self.full.at[pl.ds(0, (g - 1) * self.coarse)], sems.at[10])


def whole_kernel(
    n, pos_ref, ang_ref, obj_hbm, meas_hbm, prb_hbm, fwd_hbm, inv_hbm, radial_hbm, wave_ref,
    out_ref, probe_ref,
    obj, meas, prb, fwd, inv, acc, piece, wave, mid,
    got, spread, harm, matrix, high, low, load_sems, send_a, recv_a, send_b, recv_b, *reds,
):
    me = lax.axis_index("angle")
    rows, cols = obj.shape[1:]
    patches, size = meas.shape[0], meas.shape[1]
    share, wide = rows // n, cols // CHUNKS
    loads = [
        pltpu.make_async_copy(src, dst, load_sems.at[i])
        for i, (src, dst) in enumerate((
            (obj_hbm, obj), (prb_hbm, prb), (fwd_hbm, fwd), (inv_hbm, inv), (meas_hbm, meas), (radial_hbm, matrix),
        ))
    ]
    for load in loads:
        load.start()
    greet(n, me)
    acc[...] = jnp.zeros_like(acc)
    for load in loads[:-1]:
        load.wait()

    def place(k):
        col = pos_ref[0, k, 1]
        return col, lax.rem(col, size), k // 2

    spans = [pl.ds(q * wide, wide) for q in range(CHUNKS)]
    ends = [min(patches, 2 * (wide // size) * (q + 1) + 1) for q in range(CHUNKS)]
    groups = list(zip([0] + ends[:-1], ends))
    many = len(Reduction.scratch(n, 2 * size, size))
    probe = prb
    for step in range(ITERS):
        if step < ITERS - 1:
            red = Reduction(n, me, *reds[step * many:(step + 1) * many])
        else:
            red = Nested(n, me, *reds[step * many:])
        pre, pim = probe[:size, :], probe[size:, :]
        rate = object_rate / jnp.max(pre * pre + pim * pim)
        energy = jnp.zeros((SUBLANES, size), jnp.float32)
        for q, group in enumerate(groups):
            energy = gradient_pass(
                group, place, obj, meas, probe, fwd, inv, red.pg, acc, energy, piece, wave, mid, q == 0
            )
            span = spans[q]
            obj[:, :, span] = obj[:, :, span] - rate * acc[:, :, span]
            acc[:, :, span] = jnp.zeros((2, rows, wide), jnp.float32)
            if q == CHUNKS - 1:
                red.en[...] = jnp.sum(energy, 0, keepdims=True)
                if step == 0:
                    pl.semaphore_wait(pltpu.get_barrier_semaphore(), n - 1)
                red.scatter()
            if step == ITERS - 1:
                send(n, me, lambda d: (
                    obj.at[:, rows_at(d, share), span], got.at[me, :, :, span], send_a.at[q], recv_a.at[q]
                ))
        if step < ITERS - 1:
            red.gather(probe)
            red.arrive()
            red.leave()
            probe = red.full
    got[me] = obj[:, rows_at(me, share), :]
    red.cross()
    loads[-1].wait()

    def split(i, carry):
        part = pl.ds(pl.multiple_of(i * LANES, LANES), LANES)
        value = matrix[part, :]
        top = value.astype(jnp.bfloat16)
        high[part, :] = top
        low[part, :] = (value - top.astype(jnp.float32)).astype(jnp.bfloat16)
        return carry

    lax.fori_loop(0, cols // LANES, split, 0)

    def weights(k, b):
        phase = lax.rem(k * ang_ref[b], n)
        return wave_ref[phase], wave_ref[phase + n]

    for q, span in enumerate(spans):
        drain(got.at[pl.ds(0, n - 1), :, :, span], recv_a.at[q])
        if q == CHUNKS - 1:
            red.gather(probe)

        def harmonic(k, carry):
            re = jnp.zeros((share, wide), jnp.float32)
            im = jnp.zeros((share, wide), jnp.float32)
            for b in range(n):
                wc, ws = weights(k, b)
                pr, pi = got[b, 0, :, span], got[b, 1, :, span]
                re += wc * pr + ws * pi
                im += wc * pi - ws * pr
            spread[k, 0, :, span] = re
            spread[k, 1, :, span] = im
            return carry

        lax.fori_loop(0, n, harmonic, 0)
        send(n, me, lambda d: (
            spread.at[d, :, :, span], harm.at[:, rows_at(me, share), span], send_b.at[q], recv_b.at[q]
        ))
        harm[:, rows_at(me, share), span] = spread[me, :, :, span]
    for q, span in enumerate(spans):
        drain(harm.at[:, pl.ds(0, (n - 1) * share), span], recv_b.at[q])
        value = harm[:, :, span].reshape(2 * rows, wide)
        top = value.astype(jnp.bfloat16)
        rest = (value - top.astype(jnp.float32)).astype(jnp.bfloat16)
        part = dot32(rest, high[span, :]) + dot32(top, low[span, :]) + dot32(top, high[span, :])
        if q == 0:
            out_ref[...] = part
        else:
            out_ref[...] += part
        if q == CHUNKS - 2:
            red.share()
    red.arrive()
    probe_ref[...] = red.full[...]
    red.leave()
    for q, span in enumerate(spans):
        drain(got.at[pl.ds(0, n - 1), :, :, span], send_a.at[q])
        drain(got.at[pl.ds(0, n - 1), :, :, span], send_b.at[q])


def whole_call(n, object_init, measured, positions, angle_list, probe, radial):
    rows, cols = object_init.shape[2:]
    patches, size = measured.shape[1:3]
    prows = 2 * size
    f32, bf16 = jnp.float32, jnp.bfloat16
    forward, inverse = block_tables(size)
    phase = np.arange(n).astype(np.float32) * np.float32(2.0 * math.pi / n)
    scale = np.float32(1.0 / math.sqrt(n))
    slices, probe_out = pl.pallas_call(
        functools.partial(whole_kernel, n),
        name="whole",
        out_shape=(
            jax.ShapeDtypeStruct((2 * rows, cols), f32),
            jax.ShapeDtypeStruct((prows, size), f32),
        ),
        in_specs=[SMEM_SPEC] * 2 + [HBM_SPEC] * 6 + [SMEM_SPEC],
        out_specs=(VMEM_SPEC,) * 2,
        scratch_shapes=[
            pltpu.VMEM((2, rows, cols), f32),
            pltpu.VMEM((patches, size, size), bf16),
            pltpu.VMEM((prows, size), f32),
            pltpu.VMEM((prows, prows), bf16),
            pltpu.VMEM((prows, prows), bf16),
            pltpu.VMEM((2, rows, cols), f32),
            pltpu.VMEM((patches, 2, size, size), f32),
            pltpu.VMEM((prows, patches * size), bf16),
            pltpu.VMEM((patches * size, prows), bf16),
            pltpu.VMEM((n, 2, rows // n, cols), f32),
            pltpu.VMEM((n, 2, rows // n, cols), f32),
            pltpu.VMEM((2, rows, cols), f32),
            pltpu.VMEM((cols, cols), f32),
            pltpu.VMEM((cols, cols), bf16),
            pltpu.VMEM((cols, cols), bf16),
            pltpu.SemaphoreType.DMA((6,)),
        ]
        + [pltpu.SemaphoreType.DMA((CHUNKS,))] * 4
        + Reduction.scratch(n, prows, size) * (ITERS - 1)
        + Nested.scratch(n, prows, size),
        compiler_params=pltpu.CompilerParams(
            collective_id=0, has_side_effects=True, vmem_limit_bytes=67043328
        ),
    )(
        positions, angle_list, object_init.reshape(2, rows, cols), measured.reshape(patches, size, size),
        probe.reshape(prows, size), jnp.asarray(forward), jnp.asarray(inverse), radial.reshape(cols, cols),
        jnp.asarray(np.concatenate([np.cos(phase), np.sin(phase)]) * scale),
    )
    return slices.reshape(object_init.shape), probe_out.reshape(probe.shape)


def tables(count, index_list):
    cosine_part, sine_part = tables_exact(count, index_list)
    return (cosine_part.astype(jnp.bfloat16), sine_part.astype(jnp.bfloat16))


def left(table, field):
    return jnp.einsum("jk,nkl->njl", table, field, preferred_element_type=jnp.float32)


def right(field, table):
    return jnp.einsum("njk,kl->njl", field, table, preferred_element_type=jnp.float32)


def gradient_list(
    object_field, measured_intensity, scan_positions, probe_field, cosine_theta, sine_theta
):
    size = probe_field.shape[1]
    zero_index = jnp.zeros((), jnp.int32)
    pieces = jax.vmap(
        lambda row, col: lax.dynamic_slice(object_field, (zero_index, row, col), (2, size, size))
    )(scan_positions[:, 0], scan_positions[:, 1])
    piece_re, piece_im = (pieces[:, 0], pieces[:, 1])
    probe_re, probe_im = (probe_field[0], probe_field[1])
    wave_re = (probe_re * piece_re - probe_im * piece_im).astype(jnp.bfloat16)
    wave_im = (probe_re * piece_im + probe_im * piece_re).astype(jnp.bfloat16)
    half_re = (left(cosine_theta, wave_re) + left(sine_theta, wave_im)).astype(jnp.bfloat16)
    half_im = (left(cosine_theta, wave_im) - left(sine_theta, wave_re)).astype(jnp.bfloat16)
    farfield_real = right(half_re, cosine_theta) + right(half_im, sine_theta)
    farfield_imaginary = right(half_im, cosine_theta) - right(half_re, sine_theta)
    residual_error = (
        farfield_real * farfield_real
        + farfield_imaginary * farfield_imaginary
        - measured_intensity.astype(jnp.float32)
    )
    push_re = (residual_error * farfield_real).astype(jnp.bfloat16)
    push_im = (residual_error * farfield_imaginary).astype(jnp.bfloat16)
    back_re = (left(cosine_theta, push_re) - left(sine_theta, push_im)).astype(jnp.bfloat16)
    back_im = (left(cosine_theta, push_im) + left(sine_theta, push_re)).astype(jnp.bfloat16)
    grad_re = right(back_re, cosine_theta) - right(back_im, sine_theta)
    grad_im = right(back_im, cosine_theta) + right(back_re, sine_theta)
    step_re = probe_re * grad_re + probe_im * grad_im
    step_im = probe_re * grad_im - probe_im * grad_re
    steps_all = jnp.stack([step_re, step_im], 1)

    def place(index, total):
        start = (zero_index, scan_positions[index, 0], scan_positions[index, 1])
        current = lax.dynamic_slice(total, start, (2, size, size))
        return lax.dynamic_update_slice(total, current + steps_all[index], start)

    obj_grad = lax.fori_loop(0, scan_positions.shape[0], place, jnp.zeros_like(object_field))
    pg_re = jnp.sum(piece_re * grad_re + piece_im * grad_im, 0)
    pg_im = jnp.sum(piece_re * grad_im - piece_im * grad_re, 0)
    energy = jnp.sum(piece_re * piece_re + piece_im * piece_im)
    return (obj_grad, jnp.stack([pg_re, pg_im], 0), energy)


def angular(block, wave_cos, wave_sin):
    count = block.shape[0]
    flat = block.reshape(count, -1)
    exact = lax.Precision.HIGHEST
    part_cos = jnp.dot(wave_cos, flat, precision=exact, preferred_element_type=jnp.float32).reshape(
        block.shape
    )
    part_sin = jnp.dot(wave_sin, flat, precision=exact, preferred_element_type=jnp.float32).reshape(
        block.shape
    )
    harm_re = part_cos[:, 0] + part_sin[:, 1]
    harm_im = part_cos[:, 1] - part_sin[:, 0]
    return jnp.stack([harm_re, harm_im], 1)


def plain_device(object_init, measured, positions, angle_list, probe, radial):
    size = probe.shape[1]
    cosine_theta, sine_theta = tables(size, jnp.arange(size, dtype=jnp.int32))
    object_field = object_init
    probe_field = probe
    for step in range(ITERS):

        def one(items):
            return gradient_list(
                items[0], items[1], items[2], probe_field, cosine_theta, sine_theta
            )

        obj_grads, probe_grads, energies = lax.map(one, (object_field, measured, positions))
        probe_total, energy_total = lax.psum((jnp.sum(probe_grads, 0), jnp.sum(energies)), "angle")
        peak = jnp.max(probe_field[0] * probe_field[0] + probe_field[1] * probe_field[1])
        object_field = object_field - object_rate / peak * obj_grads
        probe_field = probe_field - probe_rate * probe_total / (energy_total / (size * size))
    wave_cos, wave_sin = tables_exact(angle_list.shape[0], angle_list)
    gathered = lax.all_to_all(object_field, "angle", split_axis=2, concat_axis=0, tiled=True)
    harm = lax.all_to_all(
        angular(gathered, wave_cos, wave_sin), "angle", split_axis=0, concat_axis=2, tiled=True
    )
    slices = jnp.einsum(
        "kcrn,knm->kcrm",
        harm,
        radial,
        precision=lax.Precision.HIGHEST,
        preferred_element_type=jnp.float32,
    )
    return (slices, probe_field)


def on_device(n, object_init, measured, positions, angle_list, probe, radial):
    rows, cols = object_init.shape[2:]
    patches, size = measured.shape[1:3]
    fits = (
        object_init.shape[0] == 1
        and radial.shape[0] == 1
        and angle_list.shape[0] == n
        and rows == size == LANES
        and cols % (LANES * CHUNKS) == 0
        and patches == 2 * cols // size - 1
        and rows % (n * SUBLANES) == 0
        and n % GROUP == 0
        and n > GROUP
    )
    device = functools.partial(whole_call, n) if fits else plain_device
    return device(object_init, measured, positions, angle_list, probe, radial)


def solution(mesh):
    in_specs = (
        P(("scan", "angle"), None, None, None),
        P(("scan", "angle"), None, None, None),
        P(("scan", "angle"), None, None),
        P("scan"),
        P("scan", None, None),
        P("angle", None, None),
    )
    out_specs = (P(("scan", "angle"), None, None, None), P("scan", None, None))
    return jax.shard_map(
        functools.partial(on_device, mesh.shape["angle"]),
        mesh=mesh, in_specs=in_specs, out_specs=out_specs, check_vma=False,
    )
```
